32 devices in a mesh: gx: 4 (over z), gy: 8 (over y, x, core).
Axes of the slice: x: 2, y: 2, z: 4, core: 2. Of those that a mesh axis runs over, the one named last changes fastest.
Arguments:
- spectrum: float32 [2, 256, 16384], P(None, ('gx', 'gy')), may hold values from -6 to 6
- parameters: float32 [2], replicated, may hold values from -1.5 to 1.5
Outputs:
- advanced: float32 [2, 256, 16384], P(None, ('gx', 'gy'))
The draws below stay inside these ranges and needn't reach their ends.
All inputs are finite; a program needn't handle non-finite values.
Results may differ from the reference program's by a relative error of at most 0.0003.
Values sent between devices are 32-bit elements; how exact they have to be, the bound alone decides.
A program may use at most 128 MiB of HBM per device.

```python
import math
import jax
import jax.numpy as jnp

COLS = 16384
STEPS = 1
ROWS = 256


def levels(own_key, shape, pieces, least, largest):
    factor_of, own = 1.0, jax.random.fold_in(own_key, 6)
    for dim, parts in pieces:
        draws = jnp.exp(jax.random.uniform(jax.random.fold_in(own, dim), (parts,), jnp.float32, least / len(pieces), largest / len(pieces)))
        factor_of = factor_of * jnp.repeat(draws, shape[dim] // parts).reshape([-1 if axis == dim else 1 for axis in range(len(shape))])
    return factor_of


def scatter_about(own_key, extent, deviation, limit, pieces=(), held_as=jnp.bfloat16):
    factor_of = levels(own_key, extent, pieces, -0.22, 0.18) if pieces else 1.0
    array = jax.random.normal(own_key, extent, jnp.float32) * deviation * factor_of
    return jnp.minimum(jnp.maximum(array, -limit), limit).astype(held_as)


def setup_inputs(seed: int = 0) -> dict:
    seeds = jax.random.split(jax.random.key(seed), 3)
    return {
        "spectrum": scatter_about(seeds[0], (2, ROWS, COLS), 1.0, 6.0, ((1, 32),), jnp.float32),
        "parameters": jnp.clip(jax.random.uniform(seeds[1], (2,), jnp.float32, -1.5, 1.5), -1.5, 1.5),
    }


time_step = 0.1
spacing = 0.25


def phi_series(zeta):
    result = []
    for phi_order in (1, 2, 3):
        running = jnp.full_like(zeta, 1.0 / math.factorial(14 + phi_order))
        for degree in range(13, -1, -1):
            running = running * zeta + 1.0 / math.factorial(degree + phi_order)
        result.append(running)
    return result


def phi_values(zeta):
    inside = zeta.real * zeta.real + zeta.imag * zeta.imag < 1.0
    guarded = jnp.where(inside, jnp.ones_like(zeta), zeta)
    series = phi_series(zeta)
    phi_one = (jnp.exp(guarded) - 1.0) / guarded
    phi_two = (phi_one - 1.0) / guarded
    phi_three = (phi_two - 0.5) / guarded
    direct = [phi_one, phi_two, phi_three]
    return [jnp.where(inside, series[index], direct[index]) for index in range(3)]


def reference(spectrum, parameters):
    rows_all = spectrum.shape[1]
    columns = spectrum.shape[2]
    modes_total = rows_all * columns
    current = (spectrum[0] + 1j * spectrum[1]).reshape(modes_total)
    mode_index = jnp.arange(modes_total, dtype=jnp.int32)
    signed = jnp.where(mode_index < modes_total // 2, mode_index, mode_index - modes_total).astype(spectrum.dtype)
    wavenum = signed * (2.0 * math.pi / (modes_total * spacing))
    wave_square = wavenum * wavenum
    dispersion = parameters[0]
    cubic_twist = parameters[1]
    zeta = time_step * (1.0 - wave_square) - 1j * (time_step * dispersion * wave_square)
    phi_one, phi_two, phi_three = phi_values(zeta)
    half_weight = 0.5 * time_step * phi_values(zeta / 2.0)[0]
    decay_full = jnp.exp(zeta)
    decay_half = jnp.exp(zeta / 2.0)
    weight_one = time_step * (phi_one - 3.0 * phi_two + 4.0 * phi_three)
    weight_two = time_step * (phi_two - 2.0 * phi_three)
    weight_three = time_step * (4.0 * phi_three - phi_two)

    def nonlinear(spectral):
        physical = jnp.fft.ifft(spectral, norm="ortho")
        magnitude = physical.real * physical.real + physical.imag * physical.imag
        cubic = -(1.0 + 1j * cubic_twist) * magnitude * physical
        return jnp.fft.fft(cubic, norm="ortho")

    for repeat in range(STEPS):
        start_term = nonlinear(current)
        inner_one = decay_half * current + half_weight * start_term
        one_term = nonlinear(inner_one)
        inner_two = decay_half * current + half_weight * one_term
        two_term = nonlinear(inner_two)
        inner_three = decay_half * inner_one + half_weight * (2.0 * two_term - start_term)
        three_term = nonlinear(inner_three)
        current = (decay_full * current + weight_one * start_term
                   + 2.0 * weight_two * (one_term + two_term) + weight_three * three_term)
    return jnp.stack([current.real, current.imag]).reshape(2, rows_all, columns)
```

```python
import functools
import math

import jax
import jax.numpy as jnp
import numpy as np
from jax import lax
from jax.experimental import pallas as pl
from jax.experimental.pallas import tpu as pltpu
from jax.sharding import PartitionSpec as P

time_step = 0.1
spacing = 0.25
lanes = 128
sublanes = 8
groups = 2
height = sublanes // groups


def real_form(matrix):
    return np.block([[matrix.real, -matrix.imag], [matrix.imag, matrix.real]])


def halves(matrix):
    high = jnp.asarray(matrix, jnp.float32).astype(jnp.bfloat16)
    low = (jnp.asarray(matrix, jnp.float32) - high.astype(jnp.float32)).astype(jnp.bfloat16)
    return high, low


def unit_roots(left, right, length):
    product = (left[:, None].astype(np.int64) * right[None, :].astype(np.int64)) % length
    return np.exp(2j * np.pi * product / length)


def split(value):
    high = value.astype(jnp.bfloat16)
    return high, (value - high.astype(jnp.float32)).astype(jnp.bfloat16)


def dot(a, b):
    return jnp.dot(a, b, preferred_element_type=jnp.float32)


def dot3(left, right):
    return dot(left[0], right[0]) + dot(left[0], right[1]) + dot(left[1], right[0])


def times(a, b):
    return a[0] * b[0] - a[1] * b[1], a[0] * b[1] + a[1] * b[0]


def add(a, b):
    return a[0] + b[0], a[1] + b[1]


def quarter_wave(x, quarter):
    y = x * x
    sine = x + x * y * (-1.0 / 6 + y * (1.0 / 120 + y * (-1.0 / 5040 + y * (1.0 / 362880))))
    cosine = 1.0 + y * (-0.5 + y * (1.0 / 24 + y * (-1.0 / 720 + y * (1.0 / 40320 - y * (1.0 / 3628800)))))
    odd = (quarter & 1) == 1
    c = jnp.where(odd, sine, cosine)
    s = jnp.where(odd, cosine, sine)
    return (
        jnp.where(((quarter + 1) & 2) == 2, -c, c),
        jnp.where((quarter & 2) == 2, -s, s),
    )


def cos_sin_turn(fraction):
    scaled = fraction * 4.0
    near = jnp.floor(scaled + 0.5)
    return quarter_wave((scaled - near) * (0.5 * math.pi), near.astype(jnp.int32))


def cos_sin(angle):
    near = jnp.floor(angle * (2.0 / math.pi) + 0.5)
    x = angle - near * 1.5703125
    x = x - near * 4.83751296997070312e-4
    x = x - near * 7.54978942e-8
    return quarter_wave(x, near.astype(jnp.int32))


def phi_values(w, orders, growth_wave):
    inside = w[0] * w[0] + w[1] * w[1] < 1.0
    g = (jnp.where(inside, 1.0, w[0]), jnp.where(inside, 0.0, w[1]))
    inverse = 1.0 / (g[0] * g[0] + g[1] * g[1])
    inv = (g[0] * inverse, -g[1] * inverse)
    direct = []
    last = growth_wave
    for k in range(orders):
        last = times((last[0] - 1.0 / math.factorial(k), last[1]), inv)
        direct.append(last)
    running = (
        jnp.full_like(w[0], 1.0 / math.factorial(14 + orders)),
        jnp.zeros_like(w[0]),
    )
    for degree in range(13, -1, -1):
        running = times(running, w)
        running = (running[0] + 1.0 / math.factorial(degree + orders), running[1])
    series = [running]
    for k in range(orders - 1, 0, -1):
        running = times(running, w)
        running = (running[0] + 1.0 / math.factorial(k), running[1])
        series.insert(0, running)
    return [
        (jnp.where(inside, s[0], d[0]), jnp.where(inside, s[1], d[1]))
        for s, d in zip(series, direct)
    ]


def weights_at(mode, modes_total, dispersion):
    signed = jnp.where(mode < modes_total // 2, mode, mode - modes_total).astype(jnp.float32)
    wavenum = signed * (2.0 * math.pi / (modes_total * spacing))
    square = wavenum * wavenum
    zeta = (time_step * (1.0 - square), -(time_step * dispersion * square))
    half = (0.5 * zeta[0], 0.5 * zeta[1])
    grow = jnp.exp(half[0])
    c, s = cos_sin(half[1])
    e2 = (grow * c, grow * s)
    full = times(e2, e2)
    one, two, three = phi_values(zeta, 3, full)
    (half_one,) = phi_values(half, 1, e2)
    h = time_step
    q = tuple(0.5 * h * x for x in half_one)
    f1 = tuple(h * (a - 3.0 * b + 4.0 * c) for a, b, c in zip(one, two, three))
    f2 = tuple(2.0 * h * (b - 2.0 * c) for b, c in zip(two, three))
    f3 = tuple(h * (4.0 * c - b) for b, c in zip(two, three))
    return full, e2, q, f1, f2, f3


def loop(count, body):
    def wrapped(i, carry):
        body(i)
        return carry

    lax.fori_loop(0, count, wrapped, 0)


def turned(tile):
    return pltpu.roll(tile, height, 1)


def kernel(axes, sizes, constants, par_ref, spec_ref, *refs):
    Z, G, D, K, R = sizes
    C = 2 if K % 2 == 0 else 1
    pk = K // C
    A = K * D
    cols = A * lanes
    span = K * lanes
    wide = pk * lanes
    total = R * cols
    stored, out_ref = refs[:constants], refs[constants]
    held = refs[constants + 1 : 2 * constants + 1]
    (
        send_x, recv_x, send_y, recv_y, first, send_z, wts, ta, tb, acc, state, nl,
        xah, xal, xbh, xbl,
        const_sem, own_sem, first_sem, x_sem, y_sem, z_sem,
    ) = refs[2 * constants + 1 :]
    lah, lal, lbh, lbl, m2h, m2l, n2h, n2l, m3h, m3l, n3h, n3l, t2_ref = held

    zi = lax.axis_index(axes[0])
    gi = lax.axis_index(axes[1])
    me = zi * G + gi
    mesh_type = pl.DeviceIdType.MESH
    beta = par_ref[1]

    def partners(own, count):
        found = []
        for mask in range(count):
            if count & (count - 1):
                found.append(lax.rem(own + mask, count))
                continue
            other, bit = own, 1
            while bit < count:
                if mask & bit:
                    other = other + (1 - 2 * lax.rem(own // bit, 2)) * bit
                bit *= 2
            found.append(other)
        return found

    z_partner, g_partner = partners(zi, Z), partners(gi, G)

    def every_peer(act):
        for z in reversed(range(Z)):
            for g in reversed(range(G)):
                if z or g:
                    pz, pg = z_partner[z], g_partner[g]
                    act(pz, pg, pz * G + pg)

    def remote(src, dst, sems, pz, pg):
        return pltpu.make_async_remote_copy(
            src_ref=src, dst_ref=dst, send_sem=sems[0], recv_sem=sems[1],
            device_id=(pz, pg), device_id_type=mesh_type,
        )

    far = (z_partner[-1], g_partner[-1])
    others = pl.ds(0, D - 1)

    barrier = pltpu.get_barrier_semaphore()

    def greet(pz, pg, peer):
        pl.semaphore_signal(barrier, inc=1, device_id=(pz, pg), device_id_type=mesh_type)

    every_peer(greet)

    def columns(owner, c):
        return pl.ds(pl.multiple_of(owner * span + c * wide, lanes), wide)

    own_first = [
        pltpu.make_async_copy(
            spec_ref.at[:, :, columns(me, c)], first.at[c, me], own_sem.at[c]
        )
        for c in range(C)
    ]
    loads = [
        pltpu.make_async_copy(src, dst, const_sem.at[n])
        for n, (src, dst) in enumerate(zip(stored, held))
    ]
    pl.semaphore_wait(barrier, D - 1)
    for c in range(C):
        every_peer(
            lambda pz, pg, peer: remote(
                spec_ref.at[:, :, columns(peer, c)], first.at[c, me],
                (first_sem.at[0, c], first_sem.at[1, c]), pz, pg,
            ).start()
        )
    for own in own_first:
        own.start()
    for load in loads:
        load.start()

    norm = 1.0 / math.sqrt(total)
    tile_d = 2

    def tables(b):
        per = D // tile_d
        d0 = lax.rem(b, per) * tile_d
        k = lax.rem(b // per, K)
        rg = b // (per * K)
        shape = (tile_d, sublanes, lanes)
        sub = lax.broadcasted_iota(jnp.int32, shape, 1)
        low = sub >= height
        row = (d0 + lax.broadcasted_iota(jnp.int32, shape, 0)) * sublanes + rg * height
        row = row + jnp.where(low, sub - height, sub)
        col = me * span + k * lanes + lax.broadcasted_iota(jnp.int32, shape, 2)
        c, s = cos_sin_turn((row * col).astype(jnp.float32) * (1.0 / total))
        ta[rg, k, pl.ds(d0, tile_d)] = norm * c
        tb[rg, k, pl.ds(d0, tile_d)] = jnp.where(low, norm * s, -norm * s)

    loop(groups * K * D // tile_d, tables)

    rows_w = 16

    def prepare(b):
        k = lax.rem(b, K)
        r0 = pl.multiple_of(b // K * rows_w, rows_w)
        row = r0 + lax.broadcasted_iota(jnp.int32, (rows_w, lanes), 0)
        lane = lax.broadcasted_iota(jnp.int32, (rows_w, lanes), 1)
        col = me * span + k * lanes + lane
        for n, w in enumerate(weights_at(row * cols + col, total, par_ref[0])):
            wts[n, 0, k, pl.ds(r0, rows_w)] = w[0]
            wts[n, 1, k, pl.ds(r0, rows_w)] = w[1]

    rb = min(128, R)
    nb = rb // sublanes
    steps = R // rb

    def pair(ref, k, at):
        return ref[0, k, pl.ds(at, rb)], ref[1, k, pl.ds(at, rb)]

    def put(ref, k, at, value):
        ref[0, k, pl.ds(at, rb)] = value[0]
        ref[1, k, pl.ds(at, rb)] = value[1]

    def put_split(high, low, kk, at, value):
        h, l = split(value)
        high[pl.ds(at, rb), kk * lanes : (kk + 1) * lanes] = h
        low[pl.ds(at, rb), kk * lanes : (kk + 1) * lanes] = l

    def row_at(b):
        return pl.multiple_of(b * rb, rb)

    def block_at(b):
        return pl.ds(pl.multiple_of(b * nb, nb), nb)

    def fly(send, recv, sem, rg, c):
        recv[rg, c, me] = send[rg, c, me]
        every_peer(
            lambda pz, pg, peer: remote(
                send.at[rg, c, peer], recv.at[rg, c, me],
                (sem.at[0, rg, c], sem.at[1, rg, c]), pz, pg,
            ).start()
        )

    def all_of(send, recv, sem, rg, c):
        return remote(
            send.at[rg, c, others], recv.at[rg, c, others],
            (sem.at[0, rg, c], sem.at[1, rg, c]), *far,
        )

    mb = min(256, R)

    def launch(c, fresh):
        def group(rg):
            if not fresh:
                all_of(send_x, recv_x, x_sem, rg, c).wait_send()

            def body(b):
                at = pl.multiple_of(rg * R + b * mb, mb)
                y = dot3(
                    (lah[pl.ds(at, mb), :], lal[pl.ds(at, mb), :]), (xbh[...], xbl[...])
                )
                ds = pl.ds(pl.multiple_of(b * (mb // sublanes), mb // sublanes), mb // sublanes)
                for kk in range(pk):
                    tile = y[:, kk * lanes : (kk + 1) * lanes].reshape(-1, sublanes, lanes)
                    k = c * pk + kk
                    send_x[rg, c, ds, kk] = tile * ta[rg, k, ds] + turned(tile) * tb[rg, k, ds]

            loop(R // mb, body)
            fly(send_x, recv_x, x_sem, rg, c)

        loop(groups, group)

    def land(c, use):
        for rg in range(groups):
            all_of(send_y, recv_y, y_sem, rg, c).wait_recv()

            def turn(b):
                ds = block_at(b)
                for kk in range(pk):
                    tile = recv_y[rg, c, ds, kk]
                    k = c * pk + kk
                    value = tile * ta[rg, k, ds] - turned(tile) * tb[rg, k, ds]
                    at = pl.multiple_of(rg * R + b * rb, rb)
                    put_split(xah, xal, kk, at, value.reshape(rb, lanes))

            loop(steps, turn)

        def body(b):
            rows = pl.ds(pl.multiple_of(b * 2 * rb, 2 * rb), 2 * rb)
            y = dot3((lbh[rows, :], lbl[rows, :]), (xah[...], xal[...]))
            for kk in range(pk):
                at = slice(kk * lanes, (kk + 1) * lanes)
                use(c, kk, b, (y[:rb, at], y[rb:, at]))

        loop(steps, body)

    def physics(rg):
        for c in range(C):
            all_of(send_x, recv_x, x_sem, rg, c).wait_recv()
        lines_in = recv_x.at[rg].reshape(A * sublanes, lanes)
        lines_out = send_y.at[rg].reshape(A * sublanes, lanes)
        tr, ti = t2_ref[0], t2_ref[1]
        x = jnp.concatenate(
            [lines_in[pl.ds(g, 2 * A, stride=height), :] for g in range(height)], axis=1
        )
        y = dot3((m2h[...], m2l[...]), split(x))
        parts = []
        for g in range(height):
            yr = y[:A, g * lanes : (g + 1) * lanes]
            yi = y[A:, g * lanes : (g + 1) * lanes]
            parts.append(jnp.concatenate([yr * tr - yi * ti, yr * ti + yi * tr], axis=1))
        u = dot3(split(jnp.concatenate(parts, axis=0)), (m3h[...], m3l[...]))
        ur, ui = u[:, :lanes], u[:, lanes:]
        mag = -(ur * ur + ui * ui)
        cubic = jnp.concatenate([mag * (ur - beta * ui), mag * (ui + beta * ur)], axis=1)
        y = dot3(split(cubic), (n3h[...], n3l[...]))
        parts = []
        for g in range(height):
            yr = y[g * A : (g + 1) * A, :lanes]
            yi = y[g * A : (g + 1) * A, lanes:]
            parts.append(jnp.concatenate([yr * tr + yi * ti, yi * tr - yr * ti], axis=0))
        right = split(jnp.concatenate(parts, axis=1))
        count = 2 * D * pk
        for c in range(C):
            rows = pl.ds(c * count, count)
            x = dot3((n2h[rows, :], n2l[rows, :]), right)
            for g in range(height):
                lines_out[pl.ds(c * count * height + g, count, stride=height), :] = x[
                    :, g * lanes : (g + 1) * lanes
                ]
            fly(send_y, recv_y, y_sem, rg, c)

    E, E2, Q, F1, F2, F3 = range(6)

    def weight(n, k, at):
        return pair(wts.at[n], k, at)

    for load in loads:
        load.wait()
    for c in range(C):
        remote(
            first.at[c, others], first.at[c, others], (first_sem.at[0, c], first_sem.at[1, c]), *far
        ).wait_recv()
        own_first[c].wait()

        def take(b):
            ds = block_at(b)
            at = row_at(b)
            for kk in range(pk):
                for part in range(2):
                    v = first[c, ds, part, :, kk * lanes : (kk + 1) * lanes].reshape(rb, lanes)
                    state[2, part, c * pk + kk, pl.ds(at, rb)] = v
                    put_split(xbh, xbl, kk, pl.multiple_of(part * R + at, rb), v)

        loop(steps, take)
        launch(c, True)

    loop(R // rows_w * K, prepare)

    def hidden(body):
        def block(b):
            for k in range(K):
                body(k, row_at(b))

        loop(steps, block)

    def hide_start(k, at):
        v = pair(state.at[2], k, at)
        put(acc, k, at, times(weight(E, k, at), v))
        put(state.at[0], k, at, times(weight(E2, k, at), v))

    hidden(hide_start)
    for c in range(C):
        remote(
            first.at[c, others], first.at[c, others], (first_sem.at[0, c], first_sem.at[1, c]), *far
        ).wait_send()

    def stage(s):
        def rows_of(rg):
            @pl.when(s > 0)
            def _():
                for c in range(C):
                    all_of(send_y, recv_y, y_sem, rg, c).wait_send()

            physics(rg)

        loop(groups, rows_of)

        @pl.when(s < 3)
        def _():
            late = s // 2
            scale = 1.0 + late.astype(jnp.float32)

            def use(c, kk, b, n):
                k = c * pk + kk
                at = row_at(b)
                qn = times(weight(Q, k, at), n)
                base = pair(state.at[late], k, at)
                value = (base[0] + scale * qn[0], base[1] + scale * qn[1])
                put(nl, k, at, n)
                put(state.at[2], k, at, value)
                for part in range(2):
                    put_split(xbh, xbl, kk, pl.multiple_of(part * R + at, rb), value[part])

            def column(c):
                land(c, use)
                launch(c, False)

            loop(C, column)
            early = jnp.minimum(s, 1)

            def gather(k, at):
                n = pair(nl, k, at)
                put(acc, k, at, add(pair(acc, k, at), times(weight(F1 + early, k, at), n)))

            hidden(gather)

            @pl.when(s == 0)
            def _():
                def rebase(k, at):
                    qn = times(weight(Q, k, at), pair(nl, k, at))
                    ea = times(weight(E2, k, at), pair(state.at[2], k, at))
                    put(state.at[1], k, at, (ea[0] - qn[0], ea[1] - qn[1]))

                hidden(rebase)

    loop(4, stage)

    def use_last(c, kk, b, n):
        k = c * pk + kk
        at = row_at(b)
        value = add(pair(acc, k, at), times(weight(F3, k, at), n))
        for part in range(2):
            send_z[c, block_at(b), part, :, kk * lanes : (kk + 1) * lanes] = value[part].reshape(
                nb, sublanes, lanes
            )

    own_last = []
    for c in range(C):
        land(c, use_last)
        every_peer(
            lambda pz, pg, peer: remote(
                send_z.at[c, peer], out_ref.at[:, :, columns(me, c)],
                (z_sem.at[0, c], z_sem.at[1, c]), pz, pg,
            ).start()
        )
        own = pltpu.make_async_copy(
            send_z.at[c, me], out_ref.at[:, :, columns(me, c)], own_sem.at[c]
        )
        own.start()
        own_last.append(own)
    for rg in range(groups):
        for c in range(C):
            all_of(send_x, recv_x, x_sem, rg, c).wait_send()
            all_of(send_y, recv_y, y_sem, rg, c).wait_send()
    for c in range(C):
        own_last[c].wait()
        done = remote(
            send_z.at[c, others], out_ref.at[:, :, pl.ds(0, (D - 1) * wide)],
            (z_sem.at[0, c], z_sem.at[1, c]), *far,
        )
        done.wait_recv()
        done.wait_send()


def solution(mesh):
    axes = ("gx", "gy")
    Z, G = mesh.shape["gx"], mesh.shape["gy"]
    D = Z * G

    def local(spectrum, parameters):
        _, row_shard, columns = spectrum.shape
        assert row_shard == sublanes
        R = row_shard * D
        A = columns // lanes
        K = A // D
        assert K * D * lanes == columns
        C = 2 if K % 2 == 0 else 1
        pk = K // C
        counter = np.arange(R)
        rb = min(128, R)
        rows_part = np.arange(2 * R).reshape(2, D, groups, height).transpose(2, 1, 0, 3).reshape(-1)
        natural = np.arange(2 * R).reshape(2, R // rb, rb).swapaxes(0, 1).reshape(-1)
        across = real_form(unit_roots(counter, counter, R))[rows_part]
        la, lb = halves(across), halves(across.T[natural])
        order = np.arange(2 * A).reshape(2, D, C, pk).transpose(2, 1, 3, 0).reshape(-1)
        m2_full = real_form(unit_roots(np.arange(A), np.arange(A), A))[:, order]
        m2, n2 = halves(m2_full), halves(m2_full.T)
        m3_full = real_form(unit_roots(np.arange(lanes), np.arange(lanes), lanes)).T
        m3, n3 = halves(m3_full), halves(m3_full.T)
        turn = unit_roots(np.arange(A), np.arange(lanes), columns)
        t2 = jnp.asarray(np.stack([turn.real, turn.imag]), jnp.float32)
        constants = (*la, *lb, *m2, *n2, *m3, *n3, t2)
        anywhere = pl.BlockSpec(memory_space=pl.ANY)
        whole = pltpu.VMEM((K, R, lanes), jnp.float32)
        state = pltpu.VMEM((2, K, R, lanes), jnp.float32)
        blocks = pltpu.VMEM((groups, C, D, pk, sublanes, lanes), jnp.float32)
        outer = pltpu.VMEM((C, D, 2, sublanes, pk * lanes), jnp.float32)
        table = pltpu.VMEM((groups, K, D, sublanes, lanes), jnp.float32)
        half = pltpu.VMEM((2 * R, pk * lanes), jnp.bfloat16)
        return pl.pallas_call(
            functools.partial(kernel, axes, (Z, G, D, K, R), len(constants)),
            out_shape=jax.ShapeDtypeStruct(spectrum.shape, jnp.float32),
            in_specs=[pl.BlockSpec(memory_space=pltpu.SMEM)] + [anywhere] * (1 + len(constants)),
            out_specs=anywhere,
            scratch_shapes=[pltpu.VMEM(x.shape, x.dtype) for x in constants] + [
                blocks, blocks, blocks, blocks, outer, outer,
                pltpu.VMEM((6, 2, K, R, lanes), jnp.float32),
                table, table, state,
                pltpu.VMEM((3, 2, K, R, lanes), jnp.float32),
                state,
                half, half, half, half,
                pltpu.SemaphoreType.DMA((len(constants),)),
                pltpu.SemaphoreType.DMA((C,)),
                pltpu.SemaphoreType.DMA((2, C)),
                pltpu.SemaphoreType.DMA((2, groups, C)),
                pltpu.SemaphoreType.DMA((2, groups, C)),
                pltpu.SemaphoreType.DMA((2, C)),
            ],
            compiler_params=pltpu.CompilerParams(
                collective_id=0, has_side_effects=True, vmem_limit_bytes=60 * 1024 * 1024
            ),
        )(parameters, spectrum, *constants)

    return jax.shard_map(
        local,
        mesh=mesh,
        in_specs=(P(None, axes, None), P()),
        out_specs=P(None, axes, None),
        check_vma=False,
    )
```

```python
import functools
import math

import jax
import jax.numpy as jnp
import numpy as np
from jax import lax
from jax.experimental import pallas as pl
from jax.experimental.pallas import tpu as pltpu
from jax.sharding import PartitionSpec as P

time_step = 0.1
spacing = 0.25
lanes = 128
sublanes = 8
groups = 2
height = sublanes // groups


def real_form(matrix):
    return np.block([[matrix.real, -matrix.imag], [matrix.imag, matrix.real]])


def halves(matrix):
    high = jnp.asarray(matrix, jnp.float32).astype(jnp.bfloat16)
    low = (jnp.asarray(matrix, jnp.float32) - high.astype(jnp.float32)).astype(jnp.bfloat16)
    return high, low


def unit_roots(left, right, length):
    product = (left[:, None].astype(np.int64) * right[None, :].astype(np.int64)) % length
    return np.exp(2j * np.pi * product / length)


def split(value):
    high = value.astype(jnp.bfloat16)
    return high, (value - high.astype(jnp.float32)).astype(jnp.bfloat16)


def dot(a, b):
    return jnp.dot(a, b, preferred_element_type=jnp.float32)


def dot3(left, right):
    return dot(left[0], right[0]) + dot(left[0], right[1]) + dot(left[1], right[0])


def times(a, b):
    return a[0] * b[0] - a[1] * b[1], a[0] * b[1] + a[1] * b[0]


def add(a, b):
    return a[0] + b[0], a[1] + b[1]


def quarter_wave(x, quarter):
    y = x * x
    sine = x + x * y * (-1.0 / 6 + y * (1.0 / 120 + y * (-1.0 / 5040 + y * (1.0 / 362880))))
    cosine = 1.0 + y * (-0.5 + y * (1.0 / 24 + y * (-1.0 / 720 + y * (1.0 / 40320 - y * (1.0 / 3628800)))))
    odd = (quarter & 1) == 1
    c = jnp.where(odd, sine, cosine)
    s = jnp.where(odd, cosine, sine)
    return (
        jnp.where(((quarter + 1) & 2) == 2, -c, c),
        jnp.where((quarter & 2) == 2, -s, s),
    )


def cos_sin_turn(fraction):
    scaled = fraction * 4.0
    near = jnp.floor(scaled + 0.5)
    return quarter_wave((scaled - near) * (0.5 * math.pi), near.astype(jnp.int32))


def cos_sin(angle):
    near = jnp.floor(angle * (2.0 / math.pi) + 0.5)
    x = angle - near * 1.5703125
    x = x - near * 4.83751296997070312e-4
    x = x - near * 7.54978942e-8
    return quarter_wave(x, near.astype(jnp.int32))


def phi_values(w, orders, growth_wave):
    inside = w[0] * w[0] + w[1] * w[1] < 1.0
    g = (jnp.where(inside, 1.0, w[0]), jnp.where(inside, 0.0, w[1]))
    inverse = 1.0 / (g[0] * g[0] + g[1] * g[1])
    inv = (g[0] * inverse, -g[1] * inverse)
    direct = []
    last = growth_wave
    for k in range(orders):
        last = times((last[0] - 1.0 / math.factorial(k), last[1]), inv)
        direct.append(last)
    running = (
        jnp.full_like(w[0], 1.0 / math.factorial(14 + orders)),
        jnp.zeros_like(w[0]),
    )
    for degree in range(13, -1, -1):
        running = times(running, w)
        running = (running[0] + 1.0 / math.factorial(degree + orders), running[1])
    series = [running]
    for k in range(orders - 1, 0, -1):
        running = times(running, w)
        running = (running[0] + 1.0 / math.factorial(k), running[1])
        series.insert(0, running)
    return [
        (jnp.where(inside, s[0], d[0]), jnp.where(inside, s[1], d[1]))
        for s, d in zip(series, direct)
    ]


def weights_at(mode, modes_total, dispersion):
    signed = jnp.where(mode < modes_total // 2, mode, mode - modes_total).astype(jnp.float32)
    wavenum = signed * (2.0 * math.pi / (modes_total * spacing))
    square = wavenum * wavenum
    zeta = (time_step * (1.0 - square), -(time_step * dispersion * square))
    half = (0.5 * zeta[0], 0.5 * zeta[1])
    grow = jnp.exp(half[0])
    c, s = cos_sin(half[1])
    e2 = (grow * c, grow * s)
    full = times(e2, e2)
    one, two, three = phi_values(zeta, 3, full)
    (half_one,) = phi_values(half, 1, e2)
    h = time_step
    q = tuple(0.5 * h * x for x in half_one)
    f1 = tuple(h * (a - 3.0 * b + 4.0 * c) for a, b, c in zip(one, two, three))
    f2 = tuple(2.0 * h * (b - 2.0 * c) for b, c in zip(two, three))
    f3 = tuple(h * (4.0 * c - b) for b, c in zip(two, three))
    return full, e2, q, f1, f2, f3


def loop(count, body):
    def wrapped(i, carry):
        body(i)
        return carry

    lax.fori_loop(0, count, wrapped, 0)


def turned(tile):
    return pltpu.roll(tile, height, 1)


def kernel(axes, sizes, constants, par_ref, spec_ref, *refs):
    Z, G, D, K, R = sizes
    C = 2 if K % 2 == 0 else 1
    pk = K // C
    A = K * D
    cols = A * lanes
    span = K * lanes
    wide = pk * lanes
    total = R * cols
    stored, out_ref = refs[:constants], refs[constants]
    held = refs[constants + 1 : 2 * constants + 1]
    (
        send_x, recv_x, send_y, recv_y, first, send_z, wts, ta, tb, acc, state, nl,
        xah, xal, xbh, xbl,
        const_sem, own_sem, first_sem, x_sem, y_sem, z_sem,
    ) = refs[2 * constants + 1 :]
    lah, lal, lbh, lbl, m2h, m2l, n2h, n2l, m3h, m3l, n3h, n3l, t2_ref = held

    zi = lax.axis_index(axes[0])
    gi = lax.axis_index(axes[1])
    me = zi * G + gi
    mesh_type = pl.DeviceIdType.MESH
    beta = par_ref[1]

    def partners(own, count):
        found = []
        for mask in range(count):
            if count & (count - 1):
                found.append(lax.rem(own + mask, count))
                continue
            other, bit = own, 1
            while bit < count:
                if mask & bit:
                    other = other + (1 - 2 * lax.rem(own // bit, 2)) * bit
                bit *= 2
            found.append(other)
        return found

    z_partner, g_partner = partners(zi, Z), partners(gi, G)

    def every_peer(act):
        for z in sorted(range(Z), key=lambda m: (m < Z // 2, m)):
            for g in reversed(range(G)):
                if z or g:
                    pz, pg = z_partner[z], g_partner[g]
                    act(pz, pg, pz * G + pg)

    def remote(src, dst, sems, pz, pg):
        return pltpu.make_async_remote_copy(
            src_ref=src, dst_ref=dst, send_sem=sems[0], recv_sem=sems[1],
            device_id=(pz, pg), device_id_type=mesh_type,
        )

    far = (z_partner[-1], g_partner[-1])
    others = pl.ds(0, D - 1)

    barrier = pltpu.get_barrier_semaphore()

    def greet(pz, pg, peer):
        pl.semaphore_signal(barrier, inc=1, device_id=(pz, pg), device_id_type=mesh_type)

    every_peer(greet)

    def columns(owner, c):
        return pl.ds(pl.multiple_of(owner * span + c * wide, lanes), wide)

    own_first = [
        pltpu.make_async_copy(
            spec_ref.at[:, :, columns(me, c)], first.at[c, me], own_sem.at[c]
        )
        for c in range(C)
    ]
    loads = [
        pltpu.make_async_copy(src, dst, const_sem.at[n])
        for n, (src, dst) in enumerate(zip(stored, held))
    ]
    pl.semaphore_wait(barrier, D - 1)
    for c in range(C):
        every_peer(
            lambda pz, pg, peer: remote(
                spec_ref.at[:, :, columns(peer, c)], first.at[c, me],
                (first_sem.at[0, c], first_sem.at[1, c]), pz, pg,
            ).start()
        )
    for own in own_first:
        own.start()
    for load in loads:
        load.start()

    norm = 1.0 / math.sqrt(total)
    tile_d = 2

    def tables(b):
        per = D // tile_d
        d0 = lax.rem(b, per) * tile_d
        k = lax.rem(b // per, K)
        rg = b // (per * K)
        shape = (tile_d, sublanes, lanes)
        sub = lax.broadcasted_iota(jnp.int32, shape, 1)
        low = sub >= height
        row = (d0 + lax.broadcasted_iota(jnp.int32, shape, 0)) * sublanes + rg * height
        row = row + jnp.where(low, sub - height, sub)
        col = me * span + k * lanes + lax.broadcasted_iota(jnp.int32, shape, 2)
        c, s = cos_sin_turn((row * col).astype(jnp.float32) * (1.0 / total))
        ta[rg, k, pl.ds(d0, tile_d)] = norm * c
        tb[rg, k, pl.ds(d0, tile_d)] = jnp.where(low, norm * s, -norm * s)

    loop(groups * K * D // tile_d, tables)

    rows_w = 16

    def prepare(b):
        k = lax.rem(b, K)
        r0 = pl.multiple_of(b // K * rows_w, rows_w)
        row = r0 + lax.broadcasted_iota(jnp.int32, (rows_w, lanes), 0)
        lane = lax.broadcasted_iota(jnp.int32, (rows_w, lanes), 1)
        col = me * span + k * lanes + lane
        for n, w in enumerate(weights_at(row * cols + col, total, par_ref[0])):
            wts[n, 0, k, pl.ds(r0, rows_w)] = w[0]
            wts[n, 1, k, pl.ds(r0, rows_w)] = w[1]

    rb = min(128, R)
    nb = rb // sublanes
    steps = R // rb

    def pair(ref, k, at):
        return ref[0, k, pl.ds(at, rb)], ref[1, k, pl.ds(at, rb)]

    def put(ref, k, at, value):
        ref[0, k, pl.ds(at, rb)] = value[0]
        ref[1, k, pl.ds(at, rb)] = value[1]

    def put_split(high, low, kk, at, value):
        h, l = split(value)
        high[pl.ds(at, rb), kk * lanes : (kk + 1) * lanes] = h
        low[pl.ds(at, rb), kk * lanes : (kk + 1) * lanes] = l

    def row_at(b):
        return pl.multiple_of(b * rb, rb)

    def block_at(b):
        return pl.ds(pl.multiple_of(b * nb, nb), nb)

    def fly(send, recv, sem, rg, c):
        recv[rg, c, me] = send[rg, c, me]
        every_peer(
            lambda pz, pg, peer: remote(
                send.at[rg, c, peer], recv.at[rg, c, me],
                (sem.at[0, rg, c], sem.at[1, rg, c]), pz, pg,
            ).start()
        )

    def all_of(send, recv, sem, rg, c):
        return remote(
            send.at[rg, c, others], recv.at[rg, c, others],
            (sem.at[0, rg, c], sem.at[1, rg, c]), *far,
        )

    mb = min(256, R)

    def launch(c, fresh):
        def group(rg):
            if not fresh:
                all_of(send_x, recv_x, x_sem, rg, c).wait_send()

            def body(b):
                at = pl.multiple_of(rg * R + b * mb, mb)
                y = dot3(
                    (lah[pl.ds(at, mb), :], lal[pl.ds(at, mb), :]), (xbh[...], xbl[...])
                )
                ds = pl.ds(pl.multiple_of(b * (mb // sublanes), mb // sublanes), mb // sublanes)
                for kk in range(pk):
                    tile = y[:, kk * lanes : (kk + 1) * lanes].reshape(-1, sublanes, lanes)
                    k = c * pk + kk
                    send_x[rg, c, ds, kk] = tile * ta[rg, k, ds] + turned(tile) * tb[rg, k, ds]

            loop(R // mb, body)
            fly(send_x, recv_x, x_sem, rg, c)

        loop(groups, group)

    def land(c, use):
        for rg in range(groups):
            all_of(send_y, recv_y, y_sem, rg, c).wait_recv()

            def turn(b):
                ds = block_at(b)
                for kk in range(pk):
                    tile = recv_y[rg, c, ds, kk]
                    k = c * pk + kk
                    value = tile * ta[rg, k, ds] - turned(tile) * tb[rg, k, ds]
                    at = pl.multiple_of(rg * R + b * rb, rb)
                    put_split(xah, xal, kk, at, value.reshape(rb, lanes))

            loop(steps, turn)

        def body(b):
            rows = pl.ds(pl.multiple_of(b * 2 * rb, 2 * rb), 2 * rb)
            y = dot3((lbh[rows, :], lbl[rows, :]), (xah[...], xal[...]))
            for kk in range(pk):
                at = slice(kk * lanes, (kk + 1) * lanes)
                use(c, kk, b, (y[:rb, at], y[rb:, at]))

        loop(steps, body)

    def physics(rg):
        for c in range(C):
            all_of(send_x, recv_x, x_sem, rg, c).wait_recv()
        lines_in = recv_x.at[rg].reshape(A * sublanes, lanes)
        lines_out = send_y.at[rg].reshape(A * sublanes, lanes)
        tr, ti = t2_ref[0], t2_ref[1]
        x = jnp.concatenate(
            [lines_in[pl.ds(g, 2 * A, stride=height), :] for g in range(height)], axis=1
        )
        y = dot3((m2h[...], m2l[...]), split(x))
        parts = []
        for g in range(height):
            yr = y[:A, g * lanes : (g + 1) * lanes]
            yi = y[A:, g * lanes : (g + 1) * lanes]
            parts.append(jnp.concatenate([yr * tr - yi * ti, yr * ti + yi * tr], axis=1))
        u = dot3(split(jnp.concatenate(parts, axis=0)), (m3h[...], m3l[...]))
        ur, ui = u[:, :lanes], u[:, lanes:]
        mag = -(ur * ur + ui * ui)
        cubic = jnp.concatenate([mag * (ur - beta * ui), mag * (ui + beta * ur)], axis=1)
        y = dot3(split(cubic), (n3h[...], n3l[...]))
        parts = []
        for g in range(height):
            yr = y[g * A : (g + 1) * A, :lanes]
            yi = y[g * A : (g + 1) * A, lanes:]
            parts.append(jnp.concatenate([yr * tr + yi * ti, yi * tr - yr * ti], axis=0))
        right = split(jnp.concatenate(parts, axis=1))
        count = 2 * D * pk
        for c in range(C):
            rows = pl.ds(c * count, count)
            x = dot3((n2h[rows, :], n2l[rows, :]), right)
            for g in range(height):
                lines_out[pl.ds(c * count * height + g, count, stride=height), :] = x[
                    :, g * lanes : (g + 1) * lanes
                ]
            if c == 0:
                fly(send_y, recv_y, y_sem, rg, 0)

                @pl.when(rg == groups - 1)
                def _():
                    for early in range(groups - 1):
                        for later in range(1, C):
                            fly(send_y, recv_y, y_sem, early, later)
            else:

                @pl.when(rg == groups - 1)
                def _():
                    fly(send_y, recv_y, y_sem, rg, c)

    E, E2, Q, F1, F2, F3 = range(6)

    def weight(n, k, at):
        return pair(wts.at[n], k, at)

    for load in loads:
        load.wait()
    for c in range(C):
        remote(
            first.at[c, others], first.at[c, others], (first_sem.at[0, c], first_sem.at[1, c]), *far
        ).wait_recv()
        own_first[c].wait()

        def take(b):
            ds = block_at(b)
            at = row_at(b)
            for kk in range(pk):
                for part in range(2):
                    v = first[c, ds, part, :, kk * lanes : (kk + 1) * lanes].reshape(rb, lanes)
                    state[2, part, c * pk + kk, pl.ds(at, rb)] = v
                    put_split(xbh, xbl, kk, pl.multiple_of(part * R + at, rb), v)

        loop(steps, take)
        launch(c, True)

    loop(R // rows_w * K, prepare)

    def hidden(body):
        def block(b):
            for k in range(K):
                body(k, row_at(b))

        loop(steps, block)

    def hide_start(k, at):
        v = pair(state.at[2], k, at)
        put(acc, k, at, times(weight(E, k, at), v))
        put(state.at[0], k, at, times(weight(E2, k, at), v))

    hidden(hide_start)
    for c in range(C):
        remote(
            first.at[c, others], first.at[c, others], (first_sem.at[0, c], first_sem.at[1, c]), *far
        ).wait_send()

    def stage(s):
        def rows_of(rg):
            @pl.when(s > 0)
            def _():
                for c in range(C):
                    all_of(send_y, recv_y, y_sem, rg, c).wait_send()

            physics(rg)

        loop(groups, rows_of)

        @pl.when(s < 3)
        def _():
            late = s // 2
            scale = 1.0 + late.astype(jnp.float32)

            def use(c, kk, b, n):
                k = c * pk + kk
                at = row_at(b)
                qn = times(weight(Q, k, at), n)
                base = pair(state.at[late], k, at)
                value = (base[0] + scale * qn[0], base[1] + scale * qn[1])
                put(nl, k, at, n)
                put(state.at[2], k, at, value)
                for part in range(2):
                    put_split(xbh, xbl, kk, pl.multiple_of(part * R + at, rb), value[part])

            def column(c):
                land(c, use)
                launch(c, False)

            loop(C, column)
            early = jnp.minimum(s, 1)

            def gather(k, at):
                n = pair(nl, k, at)
                put(acc, k, at, add(pair(acc, k, at), times(weight(F1 + early, k, at), n)))

            hidden(gather)

            @pl.when(s == 0)
            def _():
                def rebase(k, at):
                    qn = times(weight(Q, k, at), pair(nl, k, at))
                    ea = times(weight(E2, k, at), pair(state.at[2], k, at))
                    put(state.at[1], k, at, (ea[0] - qn[0], ea[1] - qn[1]))

                hidden(rebase)

    loop(4, stage)

    def use_last(c, kk, b, n):
        k = c * pk + kk
        at = row_at(b)
        value = add(pair(acc, k, at), times(weight(F3, k, at), n))
        for part in range(2):
            send_z[c, block_at(b), part, :, kk * lanes : (kk + 1) * lanes] = value[part].reshape(
                nb, sublanes, lanes
            )

    own_last = []
    for c in range(C):
        land(c, use_last)
        every_peer(
            lambda pz, pg, peer: remote(
                send_z.at[c, peer], out_ref.at[:, :, columns(me, c)],
                (z_sem.at[0, c], z_sem.at[1, c]), pz, pg,
            ).start()
        )
        own = pltpu.make_async_copy(
            send_z.at[c, me], out_ref.at[:, :, columns(me, c)], own_sem.at[c]
        )
        own.start()
        own_last.append(own)
    for rg in range(groups):
        for c in range(C):
            all_of(send_x, recv_x, x_sem, rg, c).wait_send()
            all_of(send_y, recv_y, y_sem, rg, c).wait_send()
    for c in range(C):
        own_last[c].wait()
        done = remote(
            send_z.at[c, others], out_ref.at[:, :, pl.ds(0, (D - 1) * wide)],
            (z_sem.at[0, c], z_sem.at[1, c]), *far,
        )
        done.wait_recv()
        done.wait_send()


def solution(mesh):
    axes = ("gx", "gy")
    Z, G = mesh.shape["gx"], mesh.shape["gy"]
    D = Z * G

    def local(spectrum, parameters):
        _, row_shard, columns = spectrum.shape
        assert row_shard == sublanes
        R = row_shard * D
        A = columns // lanes
        K = A // D
        assert K * D * lanes == columns
        C = 2 if K % 2 == 0 else 1
        pk = K // C
        counter = np.arange(R)
        rb = min(128, R)
        rows_part = np.arange(2 * R).reshape(2, D, groups, height).transpose(2, 1, 0, 3).reshape(-1)
        natural = np.arange(2 * R).reshape(2, R // rb, rb).swapaxes(0, 1).reshape(-1)
        across = real_form(unit_roots(counter, counter, R))[rows_part]
        la, lb = halves(across), halves(across.T[natural])
        order = np.arange(2 * A).reshape(2, D, C, pk).transpose(2, 1, 3, 0).reshape(-1)
        m2_full = real_form(unit_roots(np.arange(A), np.arange(A), A))[:, order]
        m2, n2 = halves(m2_full), halves(m2_full.T)
        m3_full = real_form(unit_roots(np.arange(lanes), np.arange(lanes), lanes)).T
        m3, n3 = halves(m3_full), halves(m3_full.T)
        turn = unit_roots(np.arange(A), np.arange(lanes), columns)
        t2 = jnp.asarray(np.stack([turn.real, turn.imag]), jnp.float32)
        constants = (*la, *lb, *m2, *n2, *m3, *n3, t2)
        anywhere = pl.BlockSpec(memory_space=pl.ANY)
        whole = pltpu.VMEM((K, R, lanes), jnp.float32)
        state = pltpu.VMEM((2, K, R, lanes), jnp.float32)
        blocks = pltpu.VMEM((groups, C, D, pk, sublanes, lanes), jnp.float32)
        outer = pltpu.VMEM((C, D, 2, sublanes, pk * lanes), jnp.float32)
        table = pltpu.VMEM((groups, K, D, sublanes, lanes), jnp.float32)
        half = pltpu.VMEM((2 * R, pk * lanes), jnp.bfloat16)
        return pl.pallas_call(
            functools.partial(kernel, axes, (Z, G, D, K, R), len(constants)),
            out_shape=jax.ShapeDtypeStruct(spectrum.shape, jnp.float32),
            in_specs=[pl.BlockSpec(memory_space=pltpu.SMEM)] + [anywhere] * (1 + len(constants)),
            out_specs=anywhere,
            scratch_shapes=[pltpu.VMEM(x.shape, x.dtype) for x in constants] + [
                blocks, blocks, blocks, blocks, outer, outer,
                pltpu.VMEM((6, 2, K, R, lanes), jnp.float32),
                table, table, state,
                pltpu.VMEM((3, 2, K, R, lanes), jnp.float32),
                state,
                half, half, half, half,
                pltpu.SemaphoreType.DMA((len(constants),)),
                pltpu.SemaphoreType.DMA((C,)),
                pltpu.SemaphoreType.DMA((2, C)),
                pltpu.SemaphoreType.DMA((2, groups, C)),
                pltpu.SemaphoreType.DMA((2, groups, C)),
                pltpu.SemaphoreType.DMA((2, C)),
            ],
            compiler_params=pltpu.CompilerParams(
                collective_id=0, has_side_effects=True, vmem_limit_bytes=60 * 1024 * 1024
            ),
        )(parameters, spectrum, *constants)

    return jax.shard_map(
        local,
        mesh=mesh,
        in_specs=(P(None, axes, None), P()),
        out_specs=P(None, axes, None),
        check_vma=False,
    )
```
